8 devices in a mesh: seqs: 2 (over z, y), states: 4 (over x, core).
Axes of the slice: x: 2, y: 2, z: 1, core: 2. Of those that a mesh axis runs over, the one named last changes fastest.
Arguments:
- u_factor: bfloat16 [16384, 1024], P('states')
- w_factor: bfloat16 [16384, 1024], P('states')
- emission: bfloat16 [16384, 10000], P('states')
- init_prob: float32 [16384], P('states')
- tokens: int32 [32, 256], P('seqs'), parts along dimension 0
- lengths: int32 [32], P('seqs'), parts along dimension 0
Outputs:
- output 1: float32 [32], P('seqs'), parts along dimension 0
- output 2: float32 [32, 16384], P('seqs', 'states'), parts along dimension 0
There are 2 independent parts. The reference program is written for one: setup_inputs(seed, part) draws one part's arguments, and reference() takes and returns one part's arrays. A program takes and returns all parts, laid end to end along the dimension named above; an argument that names none is the same for every part.
All inputs are finite; a program needn't handle non-finite values.
Results may differ from the reference program's by a relative error of at most 0.001.
Values are sent between devices in bfloat16 or wider.
A program may use at most 1 GiB of HBM per device.

```python
import jax
import jax.numpy as jnp
from jax import lax

NUM_STATES = 16384
FEAT_RANK = 1024
VOCAB_SIZE = 10000
SEQ_BATCH = 16
NUM_STEPS = 256


def setup_inputs(seed: int = 0, part: int = 0) -> dict:
    key = jax.random.key(seed)
    key_u, key_w, key_em, key_pi = jax.random.split(key, 4)
    part_key = jax.random.fold_in(jax.random.key(seed + 1), part)
    key_tok, key_len = jax.random.split(part_key, 2)
    u_logits = 2.5 * jax.random.normal(key_u, (NUM_STATES, FEAT_RANK), jnp.float32)
    w_logits = 2.5 * jax.random.normal(key_w, (NUM_STATES, FEAT_RANK), jnp.float32)
    em_logits = 2.0 * jax.random.normal(key_em, (NUM_STATES, VOCAB_SIZE), jnp.float32)
    pi_logits = 2.0 * jax.random.normal(key_pi, (NUM_STATES,), jnp.float32)
    tokens = jax.random.randint(key_tok, (SEQ_BATCH, NUM_STEPS), 0, VOCAB_SIZE, dtype=jnp.int32)
    lengths = jax.random.randint(key_len, (SEQ_BATCH,), 1, NUM_STEPS + 1, dtype=jnp.int32)
    lengths = lengths.at[0].set(NUM_STEPS).at[1].set(1)
    return {
        "u_factor": jax.nn.softmax(u_logits, axis=1).astype(jnp.bfloat16),
        "w_factor": jax.nn.softmax(w_logits, axis=0).astype(jnp.bfloat16),
        "emission": jax.nn.softmax(em_logits, axis=1).astype(jnp.bfloat16),
        "init_prob": jax.nn.softmax(pi_logits),
        "tokens": tokens,
        "lengths": lengths,
    }


def reference(u_factor, w_factor, emission, init_prob, tokens, lengths):
    emit_first = jnp.take(emission, tokens[:, 0], axis=1).T.astype(jnp.float32)
    alpha_init = init_prob[None, :] * emit_first
    norm_init = jnp.sum(alpha_init, axis=1)
    alpha_init = alpha_init / norm_init[:, None]

    def step_fn(carry, step_in):
        alpha_prev, loglik_acc = carry
        step_tok, step_idx = step_in
        z_feat = jnp.dot(alpha_prev.astype(jnp.bfloat16), u_factor, preferred_element_type=jnp.float32)
        mixed_prob = jnp.dot(z_feat.astype(jnp.bfloat16), w_factor.T, preferred_element_type=jnp.float32)
        emit_col = jnp.take(emission, step_tok, axis=1).T.astype(jnp.float32)
        alpha_new = mixed_prob * emit_col
        row_norm = jnp.sum(alpha_new, axis=1)
        alpha_new = alpha_new / row_norm[:, None]
        active = step_idx < lengths
        alpha_next = jnp.where(active[:, None], alpha_new, alpha_prev)
        loglik_next = loglik_acc + jnp.where(active, jnp.log(row_norm), 0.0)
        return (alpha_next, loglik_next), None

    step_ids = jnp.arange(1, NUM_STEPS, dtype=jnp.int32)
    (alpha_last, loglik), _ = lax.scan(step_fn, (alpha_init, jnp.log(norm_init)), (tokens[:, 1:].T, step_ids))
    return loglik, alpha_last
```

```python
import functools

import jax
import jax.numpy as jnp
from jax import lax
from jax.experimental import pallas as pl
from jax.experimental.pallas import tpu as pltpu
from jax.sharding import PartitionSpec as P

MESH = pl.DeviceIdType.MESH
NC = 4
VR = 4
F32 = jnp.float32


def lane_sums(n):
    acc = n[:, :128]
    for k in range(1, n.shape[1] // 128):
        acc = acc + n[:, k * 128:(k + 1) * 128]
    return acc


def forward_kernel(g_hbm, v_hbm, u_ref, wt_ref, pi_ref, len_ref, ll_ref, alpha_ref,
                   gbuf, nb, mixed, zsend, zrecv, zbuf, cbuf, c0buf, c0recv, vown, vrecv,
                   gsem, zs_far, zs_near, zr, zb_s, zb_r, cs, cr, c0s, c0r, vl, vs_far, vs_near, vr):
    me = lax.axis_index("states")
    seq = lax.axis_index("seqs")
    core = lax.rem(me, 2)
    chip = me // 2
    hub = core == 1
    partner = me + 1 - 2 * core
    far_hub = (1 - chip) * 2 + 1
    src = 1 - core
    num_steps = g_hbm.shape[0]
    ch = zsend.shape[-1]

    def remote(src_ref, dst_ref, ssem, rsem, dev):
        return pltpu.make_async_remote_copy(src_ref=src_ref, dst_ref=dst_ref, send_sem=ssem, recv_sem=rsem,
                                            device_id=(seq, dev), device_id_type=MESH)

    def fetch(t, slot):
        return pltpu.make_async_copy(g_hbm.at[t], gbuf.at[slot], gsem.at[slot])

    def z_far(slot, j, who=src):
        return remote(zsend.at[slot, j], zrecv.at[slot, who, j], zs_far.at[slot, j], zr.at[slot, who, j], far_hub)

    def z_near(slot, j):
        return remote(zsend.at[slot, j], zrecv.at[slot, 2, j], zs_near.at[slot, j], zr.at[slot, 2, j], partner)

    def z_down(slot, j):
        return remote(zbuf.at[slot, j], zbuf.at[slot, j], zb_s.at[slot, j], zb_r.at[slot, j], partner)

    def c_down(slot):
        return remote(cbuf.at[slot], cbuf.at[slot], cs.at[slot], cr.at[slot], partner)

    def v_local(t, s):
        return pltpu.make_async_copy(v_hbm.at[t], vown.at[s], vl.at[s])

    def v_far(t, s, who=src):
        return remote(v_hbm.at[t], vrecv.at[s, who], vs_far.at[s], vr.at[s, who], far_hub)

    def v_near(t, s):
        return remote(v_hbm.at[t], vrecv.at[s, 2], vs_near.at[s], vr.at[s, 2], partner)

    def v_send(t):
        s = lax.rem(t, VR)
        v_local(t, s).start()
        v_far(t, s).start()
        v_near(t, s).start()

    peers = [lax.rem(me + d, 4) for d in range(1, 4)]
    barrier = pltpu.get_barrier_semaphore()
    for q in peers:
        pl.semaphore_signal(barrier, inc=1, device_id=(seq, q), device_id_type=MESH)
    fetch(0, 0).start()
    fetch(1, 1).start()
    pl.semaphore_wait(barrier, 3)
    v_send(1)
    v_send(2)
    fetch(0, 0).wait()
    n0 = pi_ref[...] * gbuf[0].astype(F32)
    c0buf[...] = lane_sums(n0)
    first = [remote(c0buf, c0recv.at[i], c0s.at[i], c0r.at[i], peers[i]) for i in range(3)]
    for cp in first:
        cp.start()
    for cp in first:
        cp.wait()
    c = jnp.sum(c0buf[...] + c0recv[0] + c0recv[1] + c0recv[2], axis=1, keepdims=True)
    a0 = n0 / c
    alpha_ref[...] = a0
    nb[...] = a0.astype(jnp.bfloat16)
    ll_ref[...] = jnp.broadcast_to(jnp.log(c), ll_ref.shape)

    def send(t):
        slot = lax.rem(t, 2)
        for j in range(NC):
            zsend[slot, j] = jnp.dot(nb[...], u_ref[:, j * ch:(j + 1) * ch], preferred_element_type=F32)
            z_far(slot, j).start()
            z_near(slot, j).start()

        @pl.when(t + 2 < num_steps)
        def _():
            v_send(t + 2)

    def receive(t):
        slot = lax.rem(t, 2)
        vslot = lax.rem(t, VR)

        @pl.when(t + 1 < num_steps)
        def _():
            fetch(t + 1, 1 - slot).start()

        v_local(t, vslot).wait()
        v_far(t, vslot).wait_send()
        v_near(t, vslot).wait_send()
        v_near(t, vslot).wait_recv()

        @pl.when(hub)
        def _():
            @pl.when(t > 1)
            def _():
                for j in range(NC):
                    z_down(1 - slot, j).wait_send()
                c_down(1 - slot).wait_send()
            for who in range(2):
                v_far(t, vslot, who).wait_recv()
            cbuf[slot] = jnp.zeros(cbuf.shape[1:], F32)

        for j in range(NC):
            @pl.when(hub)
            def _():
                z_near(slot, j).wait_recv()
                for who in range(2):
                    z_far(slot, j, who).wait_recv()
                z = (zsend[slot, j] + zrecv[slot, 2, j]) + (zrecv[slot, 0, j] + zrecv[slot, 1, j])
                zb = z.astype(jnp.bfloat16)
                zbuf[slot, j] = zb
                z_down(slot, j).start()
                cols = pl.ds(j * ch, ch)
                v = (vown[vslot, :, cols] + vrecv[vslot, 2, :, cols]) + (vrecv[vslot, 0, :, cols] + vrecv[vslot, 1, :, cols])
                cbuf[slot] = cbuf[slot] + lane_sums(zb.astype(F32) * v)
                if j == NC - 1:
                    c_down(slot).start()

            @pl.when(jnp.logical_not(hub))
            def _():
                z_near(slot, j).wait_recv()
                z_down(slot, j).wait_recv()
                if j == NC - 1:
                    c_down(slot).wait_recv()

            if j == NC - 1:
                for i in range(NC):
                    z_far(slot, i).wait_send()
                    z_near(slot, i).wait_send()
                fetch(t, slot).wait()
            part = jnp.dot(zbuf[slot, j], wt_ref[j * ch:(j + 1) * ch, :], preferred_element_type=F32)
            if j == 0:
                mixed[...] = part
            elif j < NC - 1:
                mixed[...] = mixed[...] + part
        u = mixed[...] + part
        c = jnp.sum(cbuf[slot], axis=1, keepdims=True)
        active = t < len_ref[...]
        a = jnp.where(active[:, :1], (u * gbuf[slot].astype(F32)) * (1.0 / c), alpha_ref[...])
        alpha_ref[...] = a
        nb[...] = a.astype(jnp.bfloat16)
        ll_ref[...] = ll_ref[...] + jnp.where(active, jnp.log(c), 0.0)

    send(1)

    def step(t, carry):
        receive(t)
        send(t + 1)
        return carry

    lax.fori_loop(1, num_steps - 1, step, 0)
    receive(num_steps - 1)

    @pl.when(hub)
    def _():
        slot = (num_steps - 1) % 2
        for j in range(NC):
            z_down(slot, j).wait_send()
        c_down(slot).wait_send()


def solution(mesh):
    def local_run(u_own, w_own, emit_own, prob_own, tokens, lengths):
        batch, num_steps = tokens.shape
        states, rank = u_own.shape
        ch = rank // NC
        g = jnp.take(emit_own.T, tokens.T.reshape(-1), axis=0, mode="clip")
        v = jnp.dot(g, w_own, preferred_element_type=F32).reshape(num_steps, batch, rank)
        g = g.reshape(num_steps, batch, states)
        lens = jnp.broadcast_to(lengths[:, None], (batch, 128))
        vm = pl.BlockSpec(memory_space=pltpu.VMEM)
        hbm = pl.BlockSpec(memory_space=pltpu.HBM)
        dma = pltpu.SemaphoreType.DMA
        bf16 = jnp.bfloat16
        ll, alpha = pl.pallas_call(
            forward_kernel,
            out_shape=(jax.ShapeDtypeStruct((batch, 128), F32),
                       jax.ShapeDtypeStruct((batch, states), F32)),
            in_specs=[hbm, hbm, vm, vm, vm, vm],
            out_specs=(vm, vm),
            scratch_shapes=[
                pltpu.VMEM((2, batch, states), bf16),
                pltpu.VMEM((batch, states), bf16),
                pltpu.VMEM((batch, states), F32),
                pltpu.VMEM((2, NC, batch, ch), F32),
                pltpu.VMEM((2, 3, NC, batch, ch), F32),
                pltpu.VMEM((2, NC, batch, ch), bf16),
                pltpu.VMEM((2, batch, 128), F32),
                pltpu.VMEM((batch, 128), F32),
                pltpu.VMEM((3, batch, 128), F32),
                pltpu.VMEM((VR, batch, rank), F32),
                pltpu.VMEM((VR, 3, batch, rank), F32),
                dma((2,)), dma((2, NC)), dma((2, NC)), dma((2, 3, NC)), dma((2, NC)), dma((2, NC)),
                dma((2,)), dma((2,)), dma((3,)), dma((3,)), dma((VR,)), dma((VR,)), dma((VR,)), dma((VR, 3)),
            ],
            compiler_params=pltpu.CompilerParams(
                collective_id=0, has_side_effects=True, vmem_limit_bytes=48 << 20),
            name="hmm_forward",
        )(g, v, u_own, w_own.T, prob_own[None, :], lens)
        return ll[:, 0], alpha

    return jax.shard_map(
        local_run,
        mesh=mesh,
        in_specs=(P("states", None), P("states", None), P("states", None), P("states"), P("seqs", None), P("seqs")),
        out_specs=(P("seqs"), P("seqs", "states")),
        check_vma=False,
    )
```

```python
import jax
import jax.numpy as jnp
from jax import lax
from jax.experimental import pallas as pl
from jax.experimental.pallas import tpu as pltpu
from jax.sharding import PartitionSpec as P

MESH = pl.DeviceIdType.MESH
NC = 4
RING = 4
MOVE = 2048
BLK = 128
F32 = jnp.float32
BF16 = jnp.bfloat16


def lane_sums(n):
    acc = n[:, :128]
    for k in range(1, n.shape[1] // 128):
        acc = acc + n[:, k * 128:(k + 1) * 128]
    return acc


def forward_kernel(g_hbm, v_hbm, u_hbm, wt_hbm, pi_ref, len_ref, ll_ref, alpha_ref,
                   u_ref, wt_ref, a_ref, gbuf, nb, mixed, zsend, zrecv, zbuf, cbuf, c0buf, c0recv, vown, vrecv, vsum,
                   ul, wl, um, wm, am, gl, gm_s, gm_r, zf, zn, zr, zd_s, zd_r, cd_s, cd_r, c0s, c0r, vl, vf, vn, vr):
    me = lax.axis_index("states")
    seq = lax.axis_index("seqs")
    core = lax.rem(me, 2)
    chip = me // 2
    hub = core == 1
    partner = me + 1 - 2 * core
    far_hub = (1 - chip) * 2 + 1
    num_steps, _, own = g_hbm.shape
    keep = own - MOVE
    ch = zsend.shape[-1]

    def remote(src_ref, dst_ref, ssem, rsem, dev):
        return pltpu.make_async_remote_copy(src_ref=src_ref, dst_ref=dst_ref, send_sem=ssem, recv_sem=rsem,
                                            device_id=(seq, dev), device_id_type=MESH)

    kept, moved, added = pl.ds(0, keep), pl.ds(keep, MOVE), pl.ds(own, MOVE)
    u_move = remote(u_hbm.at[moved, :], u_ref.at[added, :], um.at[0], um.at[1], partner)
    w_move = remote(wt_hbm.at[:, moved], wt_ref.at[:, added], wm.at[0], wm.at[1], partner)
    a_move = remote(a_ref.at[:, moved], a_ref.at[:, added], am.at[0], am.at[1], partner)
    a_back = remote(a_ref.at[:, added], a_ref.at[:, moved], am.at[2], am.at[3], partner)
    u_load = pltpu.make_async_copy(u_hbm, u_ref.at[pl.ds(0, own), :], ul)
    w_load = pltpu.make_async_copy(wt_hbm, wt_ref.at[:, pl.ds(0, own)], wl)

    def g_local(t):
        s = lax.rem(t, RING)
        return pltpu.make_async_copy(g_hbm.at[t], gbuf.at[s, :, pl.ds(0, own)], gl.at[s])

    def g_move(t):
        s = lax.rem(t, RING)
        return remote(g_hbm.at[t, :, moved], gbuf.at[s, :, added], gm_s.at[s], gm_r.at[s], partner)

    def z_far(slot, j, who):
        return remote(zsend.at[slot, j], zrecv.at[slot, who, j], zf.at[slot, j], zr.at[slot, who, j], far_hub)

    def z_near(slot, j):
        return remote(zsend.at[slot, j], zrecv.at[slot, 2, j], zn.at[slot, j], zr.at[slot, 2, j], partner)

    def z_down(slot, j):
        return remote(zbuf.at[slot, j], zbuf.at[slot, j], zd_s.at[slot, j], zd_r.at[slot, j], partner)

    def c_down(slot):
        return remote(cbuf.at[slot], cbuf.at[slot], cd_s.at[slot], cd_r.at[slot], partner)

    def v_local(t):
        s = lax.rem(t, RING)
        return pltpu.make_async_copy(v_hbm.at[t], vown.at[s], vl.at[s])

    def v_far(t, who):
        s = lax.rem(t, RING)
        return remote(v_hbm.at[t], vrecv.at[s, who], vf.at[s], vr.at[s, who], far_hub)

    def v_near(t):
        s = lax.rem(t, RING)
        return remote(v_hbm.at[t], vrecv.at[s, 2], vn.at[s], vr.at[s, 2], partner)

    def ahead_hub(t):
        g_local(t).start()
        v_far(t, 0).start()
        v_local(t).start()

    def ahead_even(t):
        g_local(t).start()
        g_move(t).start()
        v_near(t).start()
        v_far(t, 1).start()

    def update(t, u, n_states):
        slot = lax.rem(t, 2)
        c = jnp.sum(cbuf[slot], axis=1, keepdims=True)
        active = t < len_ref[...]
        cols = pl.ds(0, n_states)
        n = u * gbuf[lax.rem(t, RING), :, cols].astype(F32)
        a = jnp.where(active[:, :1], n * (1.0 / c), a_ref[:, cols])
        a_ref[:, cols] = a
        nb[:, cols] = a.astype(BF16)
        ll_ref[...] = ll_ref[...] + jnp.where(active, jnp.log(c), 0.0)

    def dot_w(slot, j, n_states):
        return jnp.dot(zbuf[slot, j], wt_ref[j * ch:(j + 1) * ch, :n_states], preferred_element_type=F32)

    def dot_u(j, n_states):
        return jnp.dot(nb[:, :n_states], u_ref[:n_states, pl.ds(pl.multiple_of(j * ch, ch), ch)], preferred_element_type=F32)

    peers = [lax.rem(me + d, 4) for d in range(1, 4)]
    barrier = pltpu.get_barrier_semaphore()
    for q in peers:
        pl.semaphore_signal(barrier, inc=1, device_id=(seq, q), device_id_type=MESH)
    g_local(0).start()
    u_load.start()
    w_load.start()
    pl.semaphore_wait(barrier, 3)

    @pl.when(jnp.logical_not(hub))
    def _():
        u_move.start()
        w_move.start()

    g_local(0).wait()
    n0 = pi_ref[...] * gbuf[0, :, :own].astype(F32)
    c0buf[...] = lane_sums(n0)
    first = [remote(c0buf, c0recv.at[i], c0s.at[i], c0r.at[i], peers[i]) for i in range(3)]
    for cp in first:
        cp.start()
    for cp in first:
        cp.wait()
    c = jnp.sum(c0buf[...] + c0recv[0] + c0recv[1] + c0recv[2], axis=1, keepdims=True)
    a0 = n0 / c
    a_ref[:, :own] = a0
    nb[:, :own] = a0.astype(BF16)
    ll_ref[...] = jnp.broadcast_to(jnp.log(c), ll_ref.shape)
    u_load.wait()
    w_load.wait()

    @pl.when(hub)
    def _():
        total = own + MOVE
        ahead_hub(1)
        ahead_hub(2)
        u_move.wait_recv()
        w_move.wait_recv()
        a_move.wait_recv()
        nb[:, own:] = a_ref[:, own:].astype(BF16)

        def send(t):
            slot = lax.rem(t, 2)

            def chunk(j, carry):
                zsend[slot, j] = dot_u(j, total)
                z_far(slot, j, 0).start()
                return carry

            lax.fori_loop(0, NC, chunk, 0)

            @pl.when(t + 2 < num_steps)
            def _():
                ahead_hub(t + 2)

        def receive(t):
            slot = lax.rem(t, 2)
            ring = lax.rem(t, RING)

            @pl.when(t > 1)
            def _():
                for j in range(NC):
                    z_down(1 - slot, j).wait_send()
                c_down(1 - slot).wait_send()
            v_local(t).wait()
            v_far(t, 0).wait_send()
            for who in range(2):
                v_far(t, who).wait_recv()
            v_near(t).wait_recv()
            g_local(t).wait()
            g_move(t).wait_recv()
            vsum[...] = (vown[ring] + vrecv[ring, 2]) + (vrecv[ring, 0] + vrecv[ring, 1])
            acc = None
            for j in range(NC):
                z_near(slot, j).wait_recv()
                for who in range(2):
                    z_far(slot, j, who).wait_recv()
                z = (zsend[slot, j] + zrecv[slot, 2, j]) + (zrecv[slot, 0, j] + zrecv[slot, 1, j])
                zb = z.astype(BF16)
                zbuf[slot, j] = zb
                z_down(slot, j).start()
                part = lane_sums(zb.astype(F32) * vsum[:, j * ch:(j + 1) * ch])
                acc = part if acc is None else acc + part
                if j == NC - 1:
                    cbuf[slot] = acc
                    c_down(slot).start()
                    for i in range(NC):
                        z_far(slot, i, 0).wait_send()
                u = dot_w(slot, j, total)
                if j == 0:
                    mixed[...] = u
                elif j < NC - 1:
                    mixed[...] = mixed[...] + u
            update(t, mixed[...] + u, total)

        send(1)

        def step(t, carry):
            receive(t)
            send(t + 1)
            return carry

        lax.fori_loop(1, num_steps - 1, step, 0)
        receive(num_steps - 1)
        slot = (num_steps - 1) % 2
        for j in range(NC):
            z_down(slot, j).wait_send()
        c_down(slot).wait_send()
        a_back.start()
        a_back.wait_send()

    @pl.when(jnp.logical_not(hub))
    def _():
        a_move.start()
        ahead_even(1)
        ahead_even(2)
        u_move.wait_send()
        w_move.wait_send()
        a_move.wait_send()

        def send(t):
            slot = lax.rem(t, 2)

            def chunk(j, carry):
                zsend[slot, j] = dot_u(j, keep)
                z_far(slot, j, 1).start()
                z_near(slot, j).start()
                return carry

            lax.fori_loop(0, NC, chunk, 0)

            @pl.when(t + 2 < num_steps)
            def _():
                ahead_even(t + 2)

        def receive(t):
            slot = lax.rem(t, 2)
            v_near(t).wait_send()
            v_far(t, 1).wait_send()
            g_move(t).wait_send()
            g_local(t).wait()
            for i in range(NC):
                z_far(slot, i, 1).wait_send()
                z_near(slot, i).wait_send()
            for j in range(NC):
                z_down(slot, j).wait_recv()
                if j == NC - 1:
                    c_down(slot).wait_recv()
                u = dot_w(slot, j, keep)
                if j == 0:
                    mixed[:, :keep] = u
                elif j < NC - 1:
                    mixed[:, :keep] = mixed[:, :keep] + u
            update(t, mixed[:, :keep] + u, keep)

        send(1)

        def step(t, carry):
            receive(t)
            send(t + 1)
            return carry

        lax.fori_loop(1, num_steps - 1, step, 0)
        receive(num_steps - 1)
        a_back.wait_recv()

    alpha_ref[...] = a_ref[:, :own]


def gather_kernel(row_ref, pick_ref, e_hbm, w_ref, g_ref, v_ref, buf, sem):
    i = pl.program_id(0)
    n = pl.num_programs(0)
    slot = lax.rem(i, 2)

    def start(blk, to):
        for r in range(BLK):
            row = pl.multiple_of(row_ref[blk * BLK + r], 2)
            pltpu.make_async_copy(e_hbm.at[pl.ds(row, 2), :], buf.at[to, pl.ds(2 * r, 2), :], sem.at[to]).start()

    def wait(which):
        pltpu.make_async_copy(e_hbm.at[pl.ds(0, 2 * BLK), :], buf.at[which], sem.at[which]).wait()

    @pl.when(i == 0)
    def _():
        start(0, 0)
    wait(slot)
    start(lax.rem(i + 1, n), 1 - slot)
    g_ref[...] = jnp.dot(pick_ref[...], buf[slot], preferred_element_type=F32).astype(BF16)
    v_ref[...] = jnp.dot(g_ref[...], w_ref[...], preferred_element_type=F32)

    @pl.when(i == n - 1)
    def _():
        wait(1 - slot)


def gather(tok, e, w):
    n = tok.shape[0]
    states, rank = w.shape
    spot = 2 * (jnp.arange(n) % BLK) + tok % 2
    pick = (spot[:, None] == jnp.arange(2 * BLK)[None, :]).astype(BF16)
    return pl.pallas_call(
        gather_kernel,
        grid_spec=pltpu.PrefetchScalarGridSpec(
            num_scalar_prefetch=1, grid=(n // BLK,),
            in_specs=[pl.BlockSpec((BLK, 2 * BLK), lambda i, t: (i, 0)), pl.BlockSpec(memory_space=pltpu.HBM),
                      pl.BlockSpec((states, rank), lambda i, t: (0, 0), pipeline_mode=pl.Buffered(1))],
            out_specs=[pl.BlockSpec((BLK, states), lambda i, t: (i, 0)), pl.BlockSpec((BLK, rank), lambda i, t: (i, 0))],
            scratch_shapes=[pltpu.VMEM((2, 2 * BLK, states), BF16), pltpu.SemaphoreType.DMA((2,))]),
        out_shape=[jax.ShapeDtypeStruct((n, states), BF16), jax.ShapeDtypeStruct((n, rank), F32)],
        compiler_params=pltpu.CompilerParams(vmem_limit_bytes=56 << 20),
        name="gather_rows",
    )(tok - tok % 2, pick, e, w)


def solution(mesh):
    def local_run(u_own, w_own, emit_own, prob_own, tokens, lengths):
        batch, num_steps = tokens.shape
        states, rank = u_own.shape
        ch = rank // NC
        total = states + MOVE
        g, v = gather(tokens.T.reshape(-1), emit_own.T, w_own)
        v = v.reshape(num_steps, batch, rank)
        g = g.reshape(num_steps, batch, states)
        lens = jnp.broadcast_to(lengths[:, None], (batch, 128))
        vm = pl.BlockSpec(memory_space=pltpu.VMEM)
        hbm = pl.BlockSpec(memory_space=pltpu.HBM)
        dma = pltpu.SemaphoreType.DMA
        ll, alpha = pl.pallas_call(
            forward_kernel,
            out_shape=(jax.ShapeDtypeStruct((batch, 128), F32),
                       jax.ShapeDtypeStruct((batch, states), F32)),
            in_specs=[hbm, hbm, hbm, hbm, vm, vm],
            out_specs=(vm, vm),
            scratch_shapes=[
                pltpu.VMEM((total, rank), BF16),
                pltpu.VMEM((rank, total), BF16),
                pltpu.VMEM((batch, total), F32),
                pltpu.VMEM((RING, batch, total), BF16),
                pltpu.VMEM((batch, total), BF16),
                pltpu.VMEM((batch, total), F32),
                pltpu.VMEM((2, NC, batch, ch), F32),
                pltpu.VMEM((2, 3, NC, batch, ch), F32),
                pltpu.VMEM((2, NC, batch, ch), BF16),
                pltpu.VMEM((2, batch, 128), F32),
                pltpu.VMEM((batch, 128), F32),
                pltpu.VMEM((3, batch, 128), F32),
                pltpu.VMEM((RING, batch, rank), F32),
                pltpu.VMEM((RING, 3, batch, rank), F32),
                pltpu.VMEM((batch, rank), F32),
                dma, dma, dma((2,)), dma((2,)), dma((4,)), dma((RING,)), dma((RING,)), dma((RING,)),
                dma((2, NC)), dma((2, NC)), dma((2, 3, NC)), dma((2, NC)), dma((2, NC)),
                dma((2,)), dma((2,)), dma((3,)), dma((3,)), dma((RING,)), dma((RING,)), dma((RING,)), dma((RING, 3)),
            ],
            compiler_params=pltpu.CompilerParams(
                collective_id=0, has_side_effects=True, vmem_limit_bytes=56 << 20),
            name="hmm_forward",
        )(g, v, u_own, w_own.T, prob_own[None, :], lens)
        return ll[:, 0], alpha

    return jax.shard_map(
        local_run,
        mesh=mesh,
        in_specs=(P("states", None), P("states", None), P("states", None), P("states"), P("seqs", None), P("seqs")),
        out_specs=(P("seqs"), P("seqs", "states")),
        check_vma=False,
    )
```

```python
import jax
import jax.numpy as jnp
from jax import lax
from jax.experimental import pallas as pl
from jax.experimental.pallas import tpu as pltpu
from jax.sharding import PartitionSpec as P

MESH = pl.DeviceIdType.MESH
NC = 4
RING = 4
MOVE = 2048
BLK = 128
F32 = jnp.float32
BF16 = jnp.bfloat16


def lane_sums(n):
    acc = n[:, :128]
    for k in range(1, n.shape[1] // 128):
        acc = acc + n[:, k * 128:(k + 1) * 128]
    return acc


def forward_kernel(g_hbm, v_hbm, u_hbm, wt_hbm, pi_ref, len_ref, ll_ref, alpha_ref,
                   u_ref, wt_ref, a_ref, gbuf, nb, mixed, zsend, zrecv, zbuf, cbuf, c0buf, c0recv, vown, vrecv, vsum,
                   ul, wl, um, wm, am, gl, gm_s, gm_r, zf, zn, zr, zd_s, zd_r, cd_s, cd_r, c0s, c0r, vl, vf, vn, vr):
    me = lax.axis_index("states")
    seq = lax.axis_index("seqs")
    core = lax.rem(me, 2)
    chip = me // 2
    hub = core == 1
    partner = me + 1 - 2 * core
    far_hub = (1 - chip) * 2 + 1
    num_steps, _, own = g_hbm.shape
    keep = own - MOVE
    ch = zsend.shape[-1]

    def remote(src_ref, dst_ref, ssem, rsem, dev):
        return pltpu.make_async_remote_copy(src_ref=src_ref, dst_ref=dst_ref, send_sem=ssem, recv_sem=rsem,
                                            device_id=(seq, dev), device_id_type=MESH)

    kept, moved, added = pl.ds(0, keep), pl.ds(keep, MOVE), pl.ds(own, MOVE)
    u_move = remote(u_hbm.at[moved, :], u_ref.at[added, :], um.at[0], um.at[1], partner)
    w_move = remote(wt_hbm.at[:, moved], wt_ref.at[:, added], wm.at[0], wm.at[1], partner)
    a_move = remote(a_ref.at[:, moved], a_ref.at[:, added], am.at[0], am.at[1], partner)
    a_back = remote(a_ref.at[:, added], a_ref.at[:, moved], am.at[2], am.at[3], partner)
    u_load = pltpu.make_async_copy(u_hbm, u_ref.at[pl.ds(0, own), :], ul)
    w_load = pltpu.make_async_copy(wt_hbm, wt_ref.at[:, pl.ds(0, own)], wl)

    def g_local(t):
        s = lax.rem(t, RING)
        return pltpu.make_async_copy(g_hbm.at[t], gbuf.at[s, :, pl.ds(0, own)], gl.at[s])

    def g_move(t):
        s = lax.rem(t, RING)
        return remote(g_hbm.at[t, :, moved], gbuf.at[s, :, added], gm_s.at[s], gm_r.at[s], partner)

    def z_far(slot, j, who):
        return remote(zsend.at[slot, j], zrecv.at[slot, who, j], zf.at[slot, j], zr.at[slot, who, j], far_hub)

    def z_near(slot, j):
        return remote(zsend.at[slot, j], zrecv.at[slot, 2, j], zn.at[slot, j], zr.at[slot, 2, j], partner)

    def z_down(slot, j):
        return remote(zbuf.at[slot, j], zbuf.at[slot, j], zd_s.at[slot, j], zd_r.at[slot, j], partner)

    def c_down(slot):
        return remote(cbuf.at[slot], cbuf.at[slot], cd_s.at[slot], cd_r.at[slot], partner)

    def v_local(t):
        s = lax.rem(t, RING)
        return pltpu.make_async_copy(v_hbm.at[t], vown.at[s], vl.at[s])

    def v_far(t, who):
        s = lax.rem(t, RING)
        return remote(v_hbm.at[t], vrecv.at[s, who], vf.at[s], vr.at[s, who], far_hub)

    def v_near(t):
        s = lax.rem(t, RING)
        return remote(v_hbm.at[t], vrecv.at[s, 2], vn.at[s], vr.at[s, 2], partner)

    def ahead_hub(t):
        g_local(t).start()
        v_far(t, 0).start()
        v_local(t).start()

    def ahead_even(t):
        g_local(t).start()
        g_move(t).start()
        v_near(t).start()
        v_far(t, 1).start()

    def update(t, u, n_states):
        slot = lax.rem(t, 2)
        c = jnp.sum(cbuf[slot], axis=1, keepdims=True)
        active = t < len_ref[...]
        cols = pl.ds(0, n_states)
        n = u * gbuf[lax.rem(t, RING), :, cols].astype(F32)
        a = jnp.where(active[:, :1], n * (1.0 / c), a_ref[:, cols])
        a_ref[:, cols] = a
        nb[:, cols] = a.astype(BF16)
        ll_ref[...] = ll_ref[...] + jnp.where(active, jnp.log(c), 0.0)

    def dot_w(slot, j, n_states):
        return jnp.dot(zbuf[slot, j], wt_ref[j * ch:(j + 1) * ch, :n_states], preferred_element_type=F32)

    def dot_u(j, n_states):
        return jnp.dot(nb[:, :n_states], u_ref[:n_states, pl.ds(pl.multiple_of(j * ch, ch), ch)], preferred_element_type=F32)

    peers = [lax.rem(me + d, 4) for d in range(1, 4)]
    barrier = pltpu.get_barrier_semaphore()
    for q in peers:
        pl.semaphore_signal(barrier, inc=1, device_id=(seq, q), device_id_type=MESH)
    g_local(0).start()
    u_load.start()
    w_load.start()
    pl.semaphore_wait(barrier, 3)

    @pl.when(jnp.logical_not(hub))
    def _():
        u_move.start()
        w_move.start()

    g_local(0).wait()
    n0 = pi_ref[...] * gbuf[0, :, :own].astype(F32)
    c0buf[...] = lane_sums(n0)
    first = [remote(c0buf, c0recv.at[i], c0s.at[i], c0r.at[i], peers[i]) for i in range(3)]
    for cp in first:
        cp.start()
    for cp in first:
        cp.wait()
    c = jnp.sum(c0buf[...] + c0recv[0] + c0recv[1] + c0recv[2], axis=1, keepdims=True)
    a0 = n0 / c
    a_ref[:, :own] = a0
    nb[:, :own] = a0.astype(BF16)
    ll_ref[...] = jnp.broadcast_to(jnp.log(c), ll_ref.shape)
    u_load.wait()
    w_load.wait()

    @pl.when(hub)
    def _():
        total = own + MOVE
        ahead_hub(1)
        ahead_hub(2)
        u_move.wait_recv()
        w_move.wait_recv()
        a_move.wait_recv()
        nb[:, own:] = a_ref[:, own:].astype(BF16)

        def send(t):
            slot = lax.rem(t, 2)

            def chunk(j, carry):
                zsend[slot, j] = dot_u(j, total)
                z_far(slot, j, 0).start()
                return carry

            lax.fori_loop(0, NC, chunk, 0)

            @pl.when(t + 2 < num_steps)
            def _():
                ahead_hub(t + 2)

        def receive(t):
            slot = lax.rem(t, 2)
            ring = lax.rem(t, RING)

            @pl.when(t > 1)
            def _():
                for j in range(NC):
                    z_down(1 - slot, j).wait_send()
                c_down(1 - slot).wait_send()
            v_local(t).wait()
            v_far(t, 0).wait_send()
            for who in range(2):
                v_far(t, who).wait_recv()
            v_near(t).wait_recv()
            g_local(t).wait()
            g_move(t).wait_recv()
            vsum[...] = (vown[ring] + vrecv[ring, 2]) + (vrecv[ring, 0] + vrecv[ring, 1])
            acc = None
            for j in range(NC):
                z_near(slot, j).wait_recv()
                for who in range(2):
                    z_far(slot, j, who).wait_recv()
                z = (zsend[slot, j] + zrecv[slot, 2, j]) + (zrecv[slot, 0, j] + zrecv[slot, 1, j])
                zb = z.astype(BF16)
                zbuf[slot, j] = zb
                z_down(slot, j).start()
                part = lane_sums(zb.astype(F32) * vsum[:, j * ch:(j + 1) * ch])
                acc = part if acc is None else acc + part
                if j == NC - 1:
                    cbuf[slot] = acc
                    c_down(slot).start()
                    for i in range(NC):
                        z_far(slot, i, 0).wait_send()
                u = dot_w(slot, j, total)
                if j == 0:
                    mixed[...] = u
                elif j < NC - 1:
                    mixed[...] = mixed[...] + u
            update(t, mixed[...] + u, total)

        send(1)

        def step(t, carry):
            receive(t)
            send(t + 1)
            return carry

        lax.fori_loop(1, num_steps - 1, step, 0)
        receive(num_steps - 1)
        slot = (num_steps - 1) % 2
        for j in range(NC):
            z_down(slot, j).wait_send()
        c_down(slot).wait_send()
        a_back.start()
        a_back.wait_send()

    @pl.when(jnp.logical_not(hub))
    def _():
        a_move.start()
        ahead_even(1)
        ahead_even(2)
        u_move.wait_send()
        w_move.wait_send()
        a_move.wait_send()

        def send(t):
            slot = lax.rem(t, 2)

            def pair(i, carry):
                z = jnp.dot(nb[:, :keep], u_ref[:keep, pl.ds(pl.multiple_of(i * 2 * ch, 2 * ch), 2 * ch)],
                            preferred_element_type=F32)
                for h in range(2):
                    zsend[slot, 2 * i + h] = z[:, h * ch:(h + 1) * ch]
                    z_far(slot, 2 * i + h, 1).start()
                    z_near(slot, 2 * i + h).start()
                return carry

            lax.fori_loop(0, NC // 2, pair, 0)

            @pl.when(t + 2 < num_steps)
            def _():
                ahead_even(t + 2)

        def receive(t):
            slot = lax.rem(t, 2)
            v_near(t).wait_send()
            v_far(t, 1).wait_send()
            g_move(t).wait_send()
            g_local(t).wait()
            for i in range(NC):
                z_far(slot, i, 1).wait_send()
                z_near(slot, i).wait_send()
            for j in range(NC):
                z_down(slot, j).wait_recv()
                if j == NC - 1:
                    c_down(slot).wait_recv()
                u = dot_w(slot, j, keep)
                if j == 0:
                    mixed[:, :keep] = u
                elif j < NC - 1:
                    mixed[:, :keep] = mixed[:, :keep] + u
            update(t, mixed[:, :keep] + u, keep)

        send(1)

        def step(t, carry):
            receive(t)
            send(t + 1)
            return carry

        lax.fori_loop(1, num_steps - 1, step, 0)
        receive(num_steps - 1)
        a_back.wait_recv()

    alpha_ref[...] = a_ref[:, :own]


def gather_kernel(row_ref, pick_ref, e_hbm, w_ref, g_ref, v_ref, buf, sem):
    i = pl.program_id(0)
    n = pl.num_programs(0)
    slot = lax.rem(i, 2)

    def start(blk, to):
        for r in range(BLK):
            row = pl.multiple_of(row_ref[blk * BLK + r], 2)
            pltpu.make_async_copy(e_hbm.at[pl.ds(row, 2), :], buf.at[to, pl.ds(2 * r, 2), :], sem.at[to]).start()

    def wait(which):
        pltpu.make_async_copy(e_hbm.at[pl.ds(0, 2 * BLK), :], buf.at[which], sem.at[which]).wait()

    @pl.when(i == 0)
    def _():
        start(0, 0)
    wait(slot)
    start(lax.rem(i + 1, n), 1 - slot)
    g_ref[...] = jnp.dot(pick_ref[...], buf[slot], preferred_element_type=F32).astype(BF16)
    v_ref[...] = jnp.dot(g_ref[...], w_ref[...], preferred_element_type=F32)

    @pl.when(i == n - 1)
    def _():
        wait(1 - slot)


def gather(tok, e, w):
    n = tok.shape[0]
    states, rank = w.shape
    spot = 2 * (jnp.arange(n) % BLK) + tok % 2
    pick = (spot[:, None] == jnp.arange(2 * BLK)[None, :]).astype(BF16)
    return pl.pallas_call(
        gather_kernel,
        grid_spec=pltpu.PrefetchScalarGridSpec(
            num_scalar_prefetch=1, grid=(n // BLK,),
            in_specs=[pl.BlockSpec((BLK, 2 * BLK), lambda i, t: (i, 0)), pl.BlockSpec(memory_space=pltpu.HBM),
                      pl.BlockSpec((states, rank), lambda i, t: (0, 0), pipeline_mode=pl.Buffered(1))],
            out_specs=[pl.BlockSpec((BLK, states), lambda i, t: (i, 0)), pl.BlockSpec((BLK, rank), lambda i, t: (i, 0))],
            scratch_shapes=[pltpu.VMEM((2, 2 * BLK, states), BF16), pltpu.SemaphoreType.DMA((2,))]),
        out_shape=[jax.ShapeDtypeStruct((n, states), BF16), jax.ShapeDtypeStruct((n, rank), F32)],
        compiler_params=pltpu.CompilerParams(vmem_limit_bytes=56 << 20),
        name="gather_rows",
    )(tok - tok % 2, pick, e, w)


def solution(mesh):
    def local_run(u_own, w_own, emit_own, prob_own, tokens, lengths):
        batch, num_steps = tokens.shape
        states, rank = u_own.shape
        ch = rank // NC
        total = states + MOVE
        g, v = gather(tokens.T.reshape(-1), emit_own.T, w_own)
        v = v.reshape(num_steps, batch, rank)
        g = g.reshape(num_steps, batch, states)
        lens = jnp.broadcast_to(lengths[:, None], (batch, 128))
        vm = pl.BlockSpec(memory_space=pltpu.VMEM)
        hbm = pl.BlockSpec(memory_space=pltpu.HBM)
        dma = pltpu.SemaphoreType.DMA
        ll, alpha = pl.pallas_call(
            forward_kernel,
            out_shape=(jax.ShapeDtypeStruct((batch, 128), F32),
                       jax.ShapeDtypeStruct((batch, states), F32)),
            in_specs=[hbm, hbm, hbm, hbm, vm, vm],
            out_specs=(vm, vm),
            scratch_shapes=[
                pltpu.VMEM((total, rank), BF16),
                pltpu.VMEM((rank, total), BF16),
                pltpu.VMEM((batch, total), F32),
                pltpu.VMEM((RING, batch, total), BF16),
                pltpu.VMEM((batch, total), BF16),
                pltpu.VMEM((batch, total), F32),
                pltpu.VMEM((2, NC, batch, ch), F32),
                pltpu.VMEM((2, 3, NC, batch, ch), F32),
                pltpu.VMEM((2, NC, batch, ch), BF16),
                pltpu.VMEM((2, batch, 128), F32),
                pltpu.VMEM((batch, 128), F32),
                pltpu.VMEM((3, batch, 128), F32),
                pltpu.VMEM((RING, batch, rank), F32),
                pltpu.VMEM((RING, 3, batch, rank), F32),
                pltpu.VMEM((batch, rank), F32),
                dma, dma, dma((2,)), dma((2,)), dma((4,)), dma((RING,)), dma((RING,)), dma((RING,)),
                dma((2, NC)), dma((2, NC)), dma((2, 3, NC)), dma((2, NC)), dma((2, NC)),
                dma((2,)), dma((2,)), dma((3,)), dma((3,)), dma((RING,)), dma((RING,)), dma((RING,)), dma((RING, 3)),
            ],
            compiler_params=pltpu.CompilerParams(
                collective_id=0, has_side_effects=True, vmem_limit_bytes=56 << 20),
            name="hmm_forward",
        )(g, v, u_own, w_own.T, prob_own[None, :], lens)
        return ll[:, 0], alpha

    return jax.shard_map(
        local_run,
        mesh=mesh,
        in_specs=(P("states", None), P("states", None), P("states", None), P("states"), P("seqs", None), P("seqs")),
        out_specs=(P("seqs"), P("seqs", "states")),
        check_vma=False,
    )
```
